256 devices in a mesh: band: 8 (over x, y_lo), grid: 32 (over y_hi, z, core).
Axes of the slice: x: 4, y: 4 (y_hi: 2, y_lo: 2; y = y_hi * 2 + y_lo), z: 8, core: 2. Of those that a mesh axis runs over, the one named last changes fastest.
Arguments:
- wavefunctions: bfloat16 [2048, 524288], P('band', 'grid'), may hold values from -6 to 6
- projectors: bfloat16 [2048, 8, 13, 256], P('grid'), may hold values from -0.0048828125 to 0.0048828125
- slot_atom: int32 [2048, 8], P('grid'), may hold values from -1 to 1023, as said below
- occupations: float32 [2048], P('band'), may hold values from 0.02 to 2
Outputs:
- density: float32 [1024, 13, 13], P('grid')
The draws below stay inside these ranges and needn't reach their ends.
Inputs may be any that keep to these rules, and one draw needn't show every extreme that they name: `slot_atom`: -1 marks an empty slot. Any other entry is an atom a whose owning domain a // 32 lies within 3 domains, counted around the closed cycle of 32 domains, of the domain of the block, block index // 64. In every domain some block has all 8 slots filled.
All inputs are finite; a program needn't handle non-finite values.
Results may differ from the reference program's by a relative error of at most 0.0003.
Values sent between devices are 32-bit elements; how exact they have to be, the bound alone decides.
No kernel may reach another device: no remote copies, remote signals or barrier semaphores. Data moves between devices by JAX's collectives and lax.ppermute only.
A program may use at most 64 MiB of HBM per device.

```python
import math
import jax
import jax.numpy as jnp
from jax import lax

NPROJ = 13
BLK = 256
CAP = 8
REACH = 3
NBLK = 64
ATOMS_DEV = 32
BANDS = 2048
ATOMS = 1024
BLOCKS = 2048
POINTS = 524288
N_GRID = 32


def draw_slot_atom(key, part):
    keys = jax.random.split(jax.random.fold_in(key, 71), 6)
    domain = jnp.arange(BLOCKS, dtype=jnp.int32) // NBLK
    lowest = max(CAP // 3, 1)
    crowding = jax.random.randint(keys[0], (N_GRID,), lowest, CAP + 1)
    filled = jax.random.randint(keys[1], (BLOCKS,), 0, 1 << 20) % crowding[domain] + 1
    full_block = jax.random.randint(keys[2], (N_GRID,), 0, NBLK)
    is_full = jnp.arange(BLOCKS, dtype=jnp.int32) % NBLK == full_block[domain]
    filled = jnp.where(is_full, CAP, filled)
    scores = jax.random.randint(keys[3], (BLOCKS, CAP), 0, 1 << 16) * CAP + jnp.arange(CAP, dtype=jnp.int32)[None, :]
    ranking = jnp.argsort(jnp.argsort(scores, axis=1), axis=1)
    used = ranking < filled[:, None]
    offset = jax.random.randint(keys[4], (BLOCKS, CAP), -REACH, REACH + 1)
    owner = jnp.mod(domain[:, None] + offset, N_GRID)
    local_atom = jax.random.randint(keys[5], (BLOCKS, CAP), 0, ATOMS_DEV)
    return jnp.where(used, owner * ATOMS_DEV + local_atom, -1).astype(jnp.int32)


def block_levels(own_key, shape, shards, low, largest):
    def one(position, shards_of):
        heights = jax.random.uniform(jax.random.fold_in(jax.random.fold_in(own_key, 6), position), (shards_of,), jnp.float32, low / len(shards), largest / len(shards))
        return jnp.repeat(jnp.exp(heights), shape[position] // shards_of).reshape((-1,) + (1,) * (len(shape) - position - 1))

    gain = one(*shards[0])
    for cut in shards[1:]:
        gain = gain * one(*cut)
    return gain


def gaussian(rng, extent, deviation, bound, shards=(), kind=jnp.bfloat16):
    level = block_levels(rng, extent, shards, -0.22, 0.18) if shards else 1.0
    array = jax.random.normal(rng, extent, jnp.float32) * deviation * level
    return jnp.minimum(jnp.maximum(array, -bound), bound).astype(kind)


def setup_inputs(seed: int = 0) -> dict:
    seeds = jax.random.split(jax.random.key(seed), 5)
    wavefunctions = gaussian(seeds[0], (BANDS, POINTS), 1.0, 6.0, ((0, 8), (1, 32)))
    projectors = gaussian(seeds[1], (BLOCKS, CAP, NPROJ, BLK), (BANDS * NBLK * CAP * BLK // (6 * ATOMS_DEV)) ** -0.5, 0.0048828125, ((0, 32),))
    slot_atom = draw_slot_atom(jax.random.fold_in(seeds[4], 71), 0)
    occupations = jnp.clip(jnp.exp(math.log(2.0) - 4.6051702 * jax.random.uniform(seeds[3], (BANDS,), jnp.float32) ** block_levels(seeds[3], (BANDS,), ((0, 8),), -0.2, 0.2)), 0.02, 2.0)
    return dict(wavefunctions=wavefunctions, projectors=projectors, slot_atom=slot_atom, occupations=occupations)


def reference(wavefunctions, projectors, slot_atom, occupations):
    band_total = wavefunctions.shape[0]
    domain_points = NBLK * BLK

    def domain_step(running, domain):
        columns = lax.dynamic_slice_in_dim(wavefunctions, (domain * domain_points).astype(jnp.int32), domain_points, 1)
        pieces = lax.dynamic_slice_in_dim(projectors, (domain * NBLK).astype(jnp.int32), NBLK, 0)
        slot_ids = lax.dynamic_slice_in_dim(slot_atom, (domain * NBLK).astype(jnp.int32), NBLK, 0).reshape(-1)
        grid_blocks = columns.astype(jnp.float32).reshape(band_total, NBLK, BLK)
        stacked = pieces.astype(jnp.float32).reshape(NBLK, CAP * NPROJ, BLK)
        slot_terms = jnp.einsum("ngb,gcb->gcn", grid_blocks, stacked, precision=lax.Precision.HIGHEST)
        slot_terms = slot_terms.reshape(NBLK * CAP, NPROJ * band_total)
        target = jnp.where(slot_ids >= 0, slot_ids, ATOMS).astype(jnp.int32)
        running = running + jax.ops.segment_sum(slot_terms, target, num_segments=ATOMS + 1)
        return running, None

    initial = jnp.zeros((ATOMS + 1, NPROJ * band_total), jnp.float32)
    running, unused = lax.scan(domain_step, initial, jnp.arange(N_GRID, dtype=jnp.int32))
    projections = running[:ATOMS].reshape(ATOMS, NPROJ, band_total)
    weighted = projections * occupations.reshape(1, 1, band_total)
    return jnp.einsum("ain,ajn->aij", weighted, projections, precision=lax.Precision.HIGHEST)
```

```python
import functools

import jax
import jax.numpy as jnp
from jax import lax
from jax.experimental import pallas as pl
from jax.experimental.pallas import tpu as pltpu
from jax.sharding import PartitionSpec as P

REACH = 3
ATOMS_DEV = 32
NPROJ = 13
CAP = 8
BLK = 256
CHUNK = 8
PAIRS = [(i, j) for i in range(NPROJ) for j in range(i, NPROJ)]
F32 = jnp.float32
BF16 = jnp.bfloat16


def targets(slots, domain, domains):
    half = domains // 2
    owner = slots >> 5
    rel = ((owner - domain + half) & (domains - 1)) - half
    rel = jnp.where((domain & 1) == 1, rel, -rel)
    band = jnp.where(rel < 0, -rel, jnp.where(rel > 0, rel + REACH, 0))
    return jnp.where(slots >= 0, band * ATOMS_DEV + (slots & (ATOMS_DEV - 1)), 255)


def project_kernel(
    domain_ref, slot_ref, proj_hbm, wave_hbm, own_ref, inner_ref, outer_ref, far_ref,
    wave_buf, proj_buf, hi_buf, lo_buf, wave_sem, proj_sem, *, domains,
):
    blocks = proj_hbm.shape[0]
    bands = wave_hbm.shape[0]
    chunks = blocks // CHUNK
    width = CHUNK * BLK

    def proj_copy(c):
        rows = pl.ds(c * CHUNK, CHUNK)
        return pltpu.make_async_copy(proj_hbm.at[rows], proj_buf.at[rows], proj_sem.at[c])

    def wave_copy(c):
        return pltpu.make_async_copy(
            wave_hbm.at[:, pl.ds(c * width, width)], wave_buf.at[c], wave_sem.at[c]
        )

    for c in range(chunks):
        proj_copy(c).start()
        wave_copy(c).start()

    slot_rows = targets(slot_ref[...], domain_ref[0], domains).astype(F32).astype(BF16)
    total = blocks * CAP
    spread = (
        lax.broadcasted_iota(jnp.int32, (blocks, total), 0)
        == lax.broadcasted_iota(jnp.int32, (blocks, total), 1) // CAP
    ).astype(F32).astype(BF16)
    wide = jnp.dot(slot_rows, spread, preferred_element_type=F32)
    keep = (
        lax.broadcasted_iota(jnp.int32, (CAP, total), 0)
        == lax.broadcasted_iota(jnp.int32, (CAP, total), 1) % CAP
    )
    row_of = jnp.sum(jnp.where(keep, wide, 0.0), axis=0, keepdims=True).astype(jnp.int32)

    window = (2 * REACH + 1) * ATOMS_DEV
    halves = 2
    half_slots = total // halves
    for h in range(halves):

        def one_chunk(c, carry):
            proj_copy(c).wait()
            wave_copy(c).wait()
            for q in range(CHUNK // 2):
                parts = []
                for g in (2 * q, 2 * q + 1):
                    parts.append(
                        lax.dot_general(
                            proj_buf[c * CHUNK + g],
                            wave_buf[c, :, g * BLK:(g + 1) * BLK],
                            (((1,), (1,)), ((), ())),
                            preferred_element_type=F32,
                        )
                    )
                rows = pl.ds(pl.multiple_of(c * (CHUNK * CAP) + q * 2 * CAP, 16), 2 * CAP)
                for i in range(NPROJ):
                    value = jnp.concatenate([p[i * CAP:(i + 1) * CAP] for p in parts], axis=0)
                    high = value.astype(BF16)
                    hi_buf[i, rows, :] = high
                    lo_buf[i, rows, :] = (value - high.astype(F32)).astype(BF16)
            return carry

        lax.fori_loop(h * chunks // halves, (h + 1) * chunks // halves, one_chunk, 0)
        cols = slice(h * half_slots, (h + 1) * half_slots)
        selector = (
            lax.broadcasted_iota(jnp.int32, (window, half_slots), 0) == row_of[:, cols]
        ).astype(F32).astype(BF16)
        for i in range(NPROJ):
            part = jnp.dot(selector, hi_buf[i, cols, :], preferred_element_type=F32)
            part = part + jnp.dot(selector, lo_buf[i, cols, :], preferred_element_type=F32)
            blocks_of = [part[k * ATOMS_DEV:(k + 1) * ATOMS_DEV] for k in range(2 * REACH + 1)]
            places = [(own_ref, (i,))]
            places += [(inner_ref, (k, i)) for k in range(REACH)]
            places += [(outer_ref, (k, i)) for k in range(REACH - 1)]
            places += [(far_ref, (i,))]
            for (ref, at), value in zip(places, blocks_of):
                if h == 0:
                    ref[at] = value
                else:
                    ref[at] = ref[at] + value


def project(wave, proj, slots, domain, domains):
    bands, points = wave.shape
    blocks = proj.shape[0]
    chunks = blocks // CHUNK
    block = (NPROJ, ATOMS_DEV, bands)
    vmem = pl.BlockSpec(memory_space=pltpu.VMEM)
    hbm = pl.BlockSpec(memory_space=pl.ANY)
    return pl.pallas_call(
        functools.partial(project_kernel, domains=domains),
        in_specs=[pl.BlockSpec(memory_space=pltpu.SMEM), vmem, hbm, hbm],
        out_specs=[vmem] * 4,
        out_shape=[
            jax.ShapeDtypeStruct(block, F32),
            jax.ShapeDtypeStruct((REACH,) + block, F32),
            jax.ShapeDtypeStruct((REACH - 1,) + block, F32),
            jax.ShapeDtypeStruct(block, F32),
        ],
        scratch_shapes=[
            pltpu.VMEM((chunks, bands, CHUNK * BLK), BF16),
            pltpu.VMEM((blocks, NPROJ * CAP, BLK), BF16),
            pltpu.VMEM((NPROJ, blocks * CAP, bands), BF16),
            pltpu.VMEM((NPROJ, blocks * CAP, bands), BF16),
            pltpu.SemaphoreType.DMA((chunks,)),
            pltpu.SemaphoreType.DMA((chunks,)),
        ],
        compiler_params=pltpu.CompilerParams(vmem_limit_bytes=48 * 1024 * 1024),
        name="project",
    )(domain, slots, proj, wave)


def gram_kernel(occ_ref, a_ref, b_ref, c_ref, out_ref):
    peers = out_ref.shape[0]
    occ = occ_ref[...]
    for t in range(ATOMS_DEV // 8):
        rows = slice(8 * t, 8 * t + 8)
        value = [a_ref[i, rows, :] + b_ref[i, rows, :] + c_ref[i, rows, :] for i in range(NPROJ)]
        scaled = [v * occ for v in value]
        lane = lax.broadcasted_iota(jnp.int32, (8, 128), 1)
        result = jnp.zeros((8, 128), F32)
        for p, (i, j) in enumerate(PAIRS):
            term = jnp.sum(scaled[i] * value[j], axis=1, keepdims=True)
            result = jnp.where(lane == p, term, result)
        for k in range(peers):
            out_ref[k, rows, :] = result


def gram(occ, a, b, c, peers):
    vmem = pl.BlockSpec(memory_space=pltpu.VMEM)
    return pl.pallas_call(
        gram_kernel,
        in_specs=[vmem] * 4,
        out_specs=vmem,
        out_shape=jax.ShapeDtypeStruct((peers, ATOMS_DEV, 128), F32),
        compiler_params=pltpu.CompilerParams(vmem_limit_bytes=8 * 1024 * 1024),
        name="gram",
    )(occ, a, b, c)


def unfold_kernel(in_ref, out_ref):
    total = in_ref[0]
    for k in range(1, in_ref.shape[0]):
        total = total + in_ref[k]
    padded = jnp.concatenate([total, jnp.zeros((128 - ATOMS_DEV, 128), F32)], axis=0)
    turned = jnp.transpose(padded)[:, :ATOMS_DEV]
    place = {pair: p for p, pair in enumerate(PAIRS)}
    for i in range(NPROJ):
        first = place[(i, i)]
        out_ref[i, i:NPROJ, :] = turned[first:first + NPROJ - i]
        for j in range(i + 1, NPROJ):
            out_ref[j, i:i + 1, :] = turned[first + j - i:first + j - i + 1]


def unfold(everything):
    vmem = pl.BlockSpec(memory_space=pltpu.VMEM)
    return pl.pallas_call(
        unfold_kernel,
        in_specs=[vmem],
        out_specs=vmem,
        out_shape=jax.ShapeDtypeStruct((NPROJ, NPROJ, ATOMS_DEV), F32),
        compiler_params=pltpu.CompilerParams(vmem_limit_bytes=8 * 1024 * 1024),
        name="unfold",
    )(everything)


def body(wavefunctions, projectors, slot_atom, occupations):
    band_count = wavefunctions.shape[0]
    block_count, capacity, proj_count, block_len = projectors.shape
    domains = lax.axis_size("grid")
    peers = lax.axis_size("band")
    domain = lax.axis_index("grid").astype(jnp.int32).reshape(1)
    chips = domains // 2
    stored = jnp.transpose(projectors, (0, 2, 1, 3)).reshape(
        block_count, proj_count * capacity, block_len
    )
    own, inner, outer, far = project(
        wavefunctions, stored, jnp.transpose(slot_atom), domain, domains
    )

    partner = [(i, i ^ 1) for i in range(domains)]
    along = [(2 * k + 1, (2 * k + 3) % domains) for k in range(chips)]
    along += [(2 * k, (2 * k - 2) % domains) for k in range(chips)]
    across = [(2 * k + 1, (2 * k + 2) % domains) for k in range(chips)]
    across += [(2 * k, (2 * k - 1) % domains) for k in range(chips)]

    swapped = lax.ppermute(inner, "grid", partner)
    passed = lax.ppermute(far, "grid", along)
    near = own + swapped[0]
    first = outer[0] + swapped[1]
    second = outer[1] + swapped[2]
    near, first, second = lax.optimization_barrier((near, first, second))
    final_second = lax.ppermute(second, "grid", along)
    first = first + passed
    final_first = lax.ppermute(first, "grid", across)

    occ = occupations.reshape(1, band_count)
    packed = gram(occ, near, final_second, final_first, peers)
    everything = lax.all_to_all(packed, "band", 0, 0, tiled=True)
    return jnp.transpose(unfold(everything), (2, 0, 1))


def solution(mesh):
    in_specs = (P("band", "grid"), P("grid", None, None, None), P("grid", None), P("band"))
    out_specs = P("grid", None, None)
    return jax.shard_map(body, mesh=mesh, in_specs=in_specs, out_specs=out_specs, check_vma=False)
```

```python
import functools

import jax
import jax.numpy as jnp
from jax import lax
from jax.experimental import pallas as pl
from jax.experimental.pallas import tpu as pltpu
from jax.sharding import PartitionSpec as P

REACH = 3
ATOMS_DEV = 32
NPROJ = 13
CAP = 8
BLK = 256
STRIDE = 96
PAIRS = [(i, j) for i in range(NPROJ) for j in range(i, NPROJ)]
F32 = jnp.float32
BF16 = jnp.bfloat16


def targets(slots, domain, domains):
    half = domains // 2
    owner = slots >> 5
    rel = ((owner - domain + half) & (domains - 1)) - half
    rel = jnp.where((domain & 1) == 1, rel, -rel)
    band = jnp.where(rel < 0, -rel, jnp.where(rel > 0, rel + REACH, 0))
    return jnp.where(slots >= 0, band * ATOMS_DEV + (slots & (ATOMS_DEV - 1)), 255)


def project_kernel(
    domain_ref, slot_hbm, proj_hbm, wave_hbm, own_ref, inner_ref, outer_ref, far_ref,
    slot_buf, wave_buf, proj_buf, turn_buf, term_buf, slot_sem, chunk_sem, *, domains,
):
    blocks = proj_hbm.shape[0]
    total = blocks * CAP
    sizes = chunk_sizes(blocks)
    starts = [sum(sizes[:c]) for c in range(len(sizes))]
    copies = [pltpu.make_async_copy(slot_hbm, slot_buf, slot_sem)]
    for c, (first, size) in enumerate(zip(starts, sizes)):
        rows = pl.ds(first, size)
        cols = pl.ds(first * BLK, size * BLK)
        copies.append(
            pltpu.make_async_copy(proj_hbm.at[rows], proj_buf.at[rows], chunk_sem.at[c])
        )
        copies.append(
            pltpu.make_async_copy(wave_hbm.at[:, cols], wave_buf.at[:, cols], chunk_sem.at[c])
        )
    for copy in copies:
        copy.start()

    def turn(c):
        rows = sizes[c] * (NPROJ * CAP + wave_hbm.shape[0]) // 3
        both = term_buf.at[:3, :rows, :]
        pltpu.make_async_copy(both, both, chunk_sem.at[c]).wait()
        for g in range(starts[c], starts[c] + sizes[c]):
            turn_buf[g] = wave_buf[:, g * BLK:(g + 1) * BLK].T

    parts = 4
    edges = [p * total // parts for p in range(parts + 1)]

    def multiply(c):
        for g in range(starts[c], starts[c] + sizes[c], 2):
            pair = [
                jnp.dot(proj_buf[k], turn_buf[k], preferred_element_type=F32) for k in (g, g + 1)
            ]
            part = max(p for p in range(parts) if edges[p] <= g * CAP)
            size = edges[part + 1] - edges[part]
            row = edges[part] + g * CAP
            for i in range(NPROJ):
                value = jnp.concatenate([p[i * CAP:(i + 1) * CAP] for p in pair], axis=0)
                high = value.astype(BF16)
                term_buf[i, row:row + 2 * CAP, :] = high
                term_buf[i, row + size:row + size + 2 * CAP, :] = (
                    value - high.astype(F32)
                ).astype(BF16)

    window = (2 * REACH + 1) * ATOMS_DEV

    def selectors():
        copies[0].wait()
        slot_rows = targets(slot_buf[...], domain_ref[0], domains).astype(F32).astype(BF16)
        spread = (
            lax.broadcasted_iota(jnp.int32, (blocks, total), 0)
            == lax.broadcasted_iota(jnp.int32, (blocks, total), 1) // CAP
        ).astype(F32).astype(BF16)
        wide = jnp.dot(slot_rows, spread, preferred_element_type=F32)
        keep = (
            lax.broadcasted_iota(jnp.int32, (CAP, total), 0)
            == lax.broadcasted_iota(jnp.int32, (CAP, total), 1) % CAP
        )
        row_of = jnp.sum(jnp.where(keep, wide, 0.0), axis=0, keepdims=True).astype(jnp.int32)
        return row_of

    def gather(row_of, part, kinds):
        size = edges[part + 1] - edges[part]
        one = (
            lax.broadcasted_iota(jnp.int32, (window, size), 0)
            == row_of[:, edges[part]:edges[part + 1]]
        ).astype(F32).astype(BF16)
        both = jnp.concatenate([one, one], axis=1)
        for i in kinds:
            result = jnp.dot(
                both, term_buf[i, 2 * edges[part]:2 * edges[part + 1], :],
                preferred_element_type=F32,
            )
            places = [(own_ref, (i,))]
            places += [(inner_ref, (k, i)) for k in range(REACH)]
            places += [(outer_ref, (k, i)) for k in range(REACH - 1)]
            places += [(far_ref, (i,))]
            for k, (ref, at) in enumerate(places):
                value = result[k * ATOMS_DEV:(k + 1) * ATOMS_DEV]
                ref[at] = value if part == 0 else ref[at] + value

    per_part = len(sizes) // parts
    row_of = None
    for step in range(len(sizes) + 1):
        if step < len(sizes):
            turn(step)
        if step > 0:
            multiply(step - 1)
        if step == 1:
            row_of = selectors()
        ready, turn_of = divmod(step - per_part, per_part)
        if 0 <= ready < parts - 1:
            gather(row_of, ready, range(NPROJ)[turn_of::per_part])
    gather(row_of, parts - 1, range(NPROJ))


def chunk_sizes(blocks):
    return [blocks // 8] * 8


def project(wave, proj, slots, domain, domains):
    bands, points = wave.shape
    blocks = proj.shape[0]
    chunks = len(chunk_sizes(blocks))
    block = (NPROJ, ATOMS_DEV, bands)
    vmem = pl.BlockSpec(memory_space=pltpu.VMEM)
    hbm = pl.BlockSpec(memory_space=pltpu.HBM)
    return pl.pallas_call(
        functools.partial(project_kernel, domains=domains),
        in_specs=[pl.BlockSpec(memory_space=pltpu.SMEM), hbm, hbm, hbm],
        out_specs=[vmem] * 4,
        out_shape=[
            jax.ShapeDtypeStruct(block, F32),
            jax.ShapeDtypeStruct((REACH,) + block, F32),
            jax.ShapeDtypeStruct((REACH - 1,) + block, F32),
            jax.ShapeDtypeStruct(block, F32),
        ],
        scratch_shapes=[
            pltpu.VMEM(slots.shape, jnp.int32),
            pltpu.VMEM((bands, points), BF16),
            pltpu.VMEM((blocks, NPROJ * CAP, BLK), BF16),
            pltpu.VMEM((blocks, BLK, bands), BF16),
            pltpu.VMEM((NPROJ, 2 * blocks * CAP, bands), BF16),
            pltpu.SemaphoreType.DMA,
            pltpu.SemaphoreType.DMA((chunks,)),
        ],
        compiler_params=pltpu.CompilerParams(vmem_limit_bytes=48 * 1024 * 1024),
        name="project",
    )(domain, slots, proj, wave)


def gram_kernel(occ_ref, a_ref, b_ref, c_ref, out_ref):
    peers = out_ref.shape[0]
    occ = occ_ref[...]
    lane = lax.broadcasted_iota(jnp.int32, (8, 128), 1)
    packed = [jnp.zeros((8, 128), F32) for _ in range(3)]
    for t in range(ATOMS_DEV // 8):
        rows = slice(8 * t, 8 * t + 8)
        value = [a_ref[i, rows, :] + b_ref[i, rows, :] + c_ref[i, rows, :] for i in range(NPROJ)]
        scaled = [v * occ for v in value]
        for p, (i, j) in enumerate(PAIRS):
            term = jnp.sum(scaled[i] * value[j], axis=1, keepdims=True)
            word, at = divmod(STRIDE * t + p, 128)
            packed[word] = jnp.where(lane == at, term, packed[word])
    for k in range(peers):
        for word in range(3):
            out_ref[k, :, 128 * word:128 * (word + 1)] = packed[word]


def gram(occ, a, b, c, peers):
    vmem = pl.BlockSpec(memory_space=pltpu.VMEM)
    return pl.pallas_call(
        gram_kernel,
        in_specs=[vmem] * 4,
        out_specs=vmem,
        out_shape=jax.ShapeDtypeStruct((peers, 8, 3 * 128), F32),
        compiler_params=pltpu.CompilerParams(vmem_limit_bytes=8 * 1024 * 1024),
        name="gram",
    )(occ, a, b, c)


def unfold_kernel(in_ref, out_ref):
    total = in_ref[0]
    for k in range(1, in_ref.shape[0]):
        total = total + in_ref[k]
    padded = jnp.concatenate([total, jnp.zeros((120, 3 * 128), F32)], axis=0)
    turned = jnp.transpose(padded)
    turned = jnp.concatenate(
        [turned[STRIDE * t:STRIDE * (t + 1), :8] for t in range(ATOMS_DEV // 8)], axis=1
    )
    place = {pair: p for p, pair in enumerate(PAIRS)}
    for i in range(NPROJ):
        first = place[(i, i)]
        out_ref[i, i:NPROJ, :] = turned[first:first + NPROJ - i]
        for j in range(i + 1, NPROJ):
            out_ref[j, i:i + 1, :] = turned[first + j - i:first + j - i + 1]


def unfold(everything):
    vmem = pl.BlockSpec(memory_space=pltpu.VMEM)
    return pl.pallas_call(
        unfold_kernel,
        in_specs=[vmem],
        out_specs=vmem,
        out_shape=jax.ShapeDtypeStruct((NPROJ, NPROJ, ATOMS_DEV), F32),
        compiler_params=pltpu.CompilerParams(vmem_limit_bytes=8 * 1024 * 1024),
        name="unfold",
    )(everything)


def body(wavefunctions, projectors, slot_atom, occupations):
    band_count = wavefunctions.shape[0]
    block_count, capacity, proj_count, block_len = projectors.shape
    domains = lax.axis_size("grid")
    peers = lax.axis_size("band")
    domain = lax.axis_index("grid").astype(jnp.int32).reshape(1)
    chips = domains // 2
    stored = jnp.transpose(projectors, (0, 2, 1, 3)).reshape(
        block_count, proj_count * capacity, block_len
    )
    own, inner, outer, far = project(
        wavefunctions, stored, jnp.transpose(slot_atom), domain, domains
    )

    partner = [(i, i ^ 1) for i in range(domains)]
    along = [(2 * k + 1, (2 * k + 3) % domains) for k in range(chips)]
    along += [(2 * k, (2 * k - 2) % domains) for k in range(chips)]
    across = [(2 * k + 1, (2 * k + 2) % domains) for k in range(chips)]
    across += [(2 * k, (2 * k - 1) % domains) for k in range(chips)]

    swapped = lax.ppermute(inner, "grid", partner)
    passed = lax.ppermute(far, "grid", along)
    near = own + swapped[0]
    first = outer[0] + swapped[1]
    second = outer[1] + swapped[2]
    near, first, second = lax.optimization_barrier((near, first, second))
    final_second = lax.ppermute(second, "grid", along)
    first = first + passed
    final_first = lax.ppermute(first, "grid", across)

    occ = occupations.reshape(1, band_count)
    packed = gram(occ, near, final_second, final_first, peers)
    everything = lax.all_to_all(packed, "band", 0, 0, tiled=True)
    return jnp.transpose(unfold(everything), (2, 0, 1))


def solution(mesh):
    in_specs = (P("band", "grid"), P("grid", None, None, None), P("grid", None), P("band"))
    out_specs = P("grid", None, None)
    return jax.shard_map(body, mesh=mesh, in_specs=in_specs, out_specs=out_specs, check_vma=False)
```

```python
import functools

import jax
import jax.numpy as jnp
from jax import lax
from jax.experimental import pallas as pl
from jax.experimental.pallas import tpu as pltpu
from jax.sharding import PartitionSpec as P


REACH = 3
CHUNK = 8
PARTS = 4
LANES = 128
ATOMS_DEV = 32
NPROJ = 13
CAP = 8
BLK = 256
STRIDE = 96
PAIRS = [(i, j) for i in range(NPROJ) for j in range(i, NPROJ)]
F32 = jnp.float32
BF16 = jnp.bfloat16


def targets(slots, domain, domains):
    half = domains // 2
    owner = slots >> 5
    rel = ((owner - domain + half) & (domains - 1)) - half
    rel = jnp.where((domain & 1) == 1, rel, -rel)
    band = jnp.where(rel < 0, -rel, jnp.where(rel > 0, rel + REACH, 0))
    return jnp.where(slots >= 0, band * ATOMS_DEV + (slots & (ATOMS_DEV - 1)), 255)


def project_kernel(*refs, domains, start):
    domain_ref, slot_ref, proj_hbm, wave_hbm, own_ref, inner_ref, outer_ref, far_ref = refs[-13:-5]
    proj_buf, wave_buf, turn_buf, term_buf, chunk_sem = refs[-5:]
    blocks = proj_hbm.shape[0]
    total = blocks * CAP
    chunks = blocks // CHUNK
    width = CHUNK * BLK
    for c in range(chunks):
        rows = pl.ds(c * CHUNK, CHUNK)
        cols = pl.ds(c * width, width)
        pltpu.make_async_copy(proj_hbm.at[rows], proj_buf.at[rows], chunk_sem.at[c]).start()
        pltpu.make_async_copy(
            wave_hbm.at[pl.ds(start, LANES), cols], wave_buf.at[:, cols], chunk_sem.at[c]
        ).start()

    def arrive(c):
        both = term_buf.at[:2, :CHUNK * (NPROJ * CAP + LANES) // 2, :]
        pltpu.make_async_copy(both, both, chunk_sem.at[c]).wait()

    slot_rows = targets(slot_ref[...], domain_ref[0], domains).astype(F32).astype(BF16)
    spread = (
        lax.broadcasted_iota(jnp.int32, (blocks, total), 0)
        == lax.broadcasted_iota(jnp.int32, (blocks, total), 1) // CAP
    ).astype(F32).astype(BF16)
    wide = jnp.dot(slot_rows, spread, preferred_element_type=F32)
    keep = (
        lax.broadcasted_iota(jnp.int32, (CAP, total), 0)
        == lax.broadcasted_iota(jnp.int32, (CAP, total), 1) % CAP
    )
    row_of = jnp.sum(jnp.where(keep, wide, 0.0), axis=0, keepdims=True).astype(jnp.int32)

    def turn(c):
        for g in range(c * CHUNK, (c + 1) * CHUNK):
            turn_buf[g] = wave_buf[:, g * BLK:(g + 1) * BLK].T

    size = total // PARTS

    def multiply(c):
        for g in range(c * CHUNK, (c + 1) * CHUNK, 2):
            pair = [
                jnp.dot(proj_buf[k], turn_buf[k], preferred_element_type=F32) for k in (g, g + 1)
            ]
            row = g * CAP // size * size + g * CAP
            for i in range(NPROJ):
                value = jnp.concatenate([p[i * CAP:(i + 1) * CAP] for p in pair], axis=0)
                high = value.astype(BF16)
                low = (value - high.astype(F32)).astype(BF16)
                lanes = slice(i % 2 * LANES, i % 2 * LANES + LANES)
                term_buf[i // 2, row:row + 2 * CAP, lanes] = high
                term_buf[i // 2, row + size:row + size + 2 * CAP, lanes] = low

    window = (2 * REACH + 1) * ATOMS_DEV

    def gather(part, kinds):
        one = (
            lax.broadcasted_iota(jnp.int32, (window, size), 0)
            == row_of[:, part * size:(part + 1) * size]
        ).astype(F32).astype(BF16)
        both = jnp.concatenate([one, one], axis=1)
        for duo in kinds:
            result = jnp.dot(
                both, term_buf[duo, 2 * part * size:2 * (part + 1) * size, :],
                preferred_element_type=F32,
            )
            for i in range(2 * duo, min(2 * duo + 2, NPROJ)):
                places = [(own_ref, (i,))]
                places += [(inner_ref, (k, i)) for k in range(REACH)]
                places += [(outer_ref, (k, i)) for k in range(REACH - 1)]
                places += [(far_ref, (i,))]
                lanes = slice(i % 2 * LANES, i % 2 * LANES + LANES)
                for k, (ref, at) in enumerate(places):
                    value = result[k * ATOMS_DEV:(k + 1) * ATOMS_DEV, lanes]
                    ref[at] = value if part == 0 else ref[at] + value

    per_part = chunks // PARTS
    duos = range((NPROJ + 1) // 2)
    for step in range(chunks + 1):
        if step < chunks:
            arrive(step)
            turn(step)
        if step > 0:
            multiply(step - 1)
        ready, at = divmod(step - per_part, per_part)
        if 0 <= ready < PARTS - 1:
            gather(ready, duos[at::per_part])
    gather(PARTS - 1, duos)


def project(wave, proj, slots, domain, domains, start, after=()):
    points = wave.shape[1]
    blocks = proj.shape[0]
    chunks = blocks // CHUNK
    block = (NPROJ, ATOMS_DEV, LANES)
    vmem = pl.BlockSpec(memory_space=pltpu.VMEM)
    hbm = pl.BlockSpec(memory_space=pl.ANY)
    return pl.pallas_call(
        functools.partial(project_kernel, domains=domains, start=start),
        in_specs=[hbm] * len(after) + [pl.BlockSpec(memory_space=pltpu.SMEM), vmem, hbm, hbm],
        out_specs=[vmem] * 4,
        out_shape=[
            jax.ShapeDtypeStruct(block, F32),
            jax.ShapeDtypeStruct((REACH,) + block, F32),
            jax.ShapeDtypeStruct((REACH - 1,) + block, F32),
            jax.ShapeDtypeStruct(block, F32),
        ],
        scratch_shapes=[
            pltpu.VMEM((blocks, NPROJ * CAP, BLK), BF16),
            pltpu.VMEM((LANES, points), BF16),
            pltpu.VMEM((blocks, BLK, LANES), BF16),
            pltpu.VMEM(((NPROJ + 1) // 2, 2 * blocks * CAP, 2 * LANES), BF16),
            pltpu.SemaphoreType.DMA((chunks,)),
        ],
        compiler_params=pltpu.CompilerParams(vmem_limit_bytes=50 * 1024 * 1024),
        name="project",
    )(*after, domain, slots, proj, wave)


def gram_kernel(occ_ref, *refs):
    out_ref = refs[-1]
    sides = [refs[:3], refs[3:6]]
    occ = [occ_ref[:, k * LANES:(k + 1) * LANES] for k in range(2)]
    lane = lax.broadcasted_iota(jnp.int32, (8, 128), 1)
    packed = [jnp.zeros((8, 128), F32) for _ in range(3)]
    for t in range(ATOMS_DEV // 8):
        rows = slice(8 * t, 8 * t + 8)
        value = [
            [a[i, rows, :] + b[i, rows, :] + c[i, rows, :] for i in range(NPROJ)]
            for a, b, c in sides
        ]
        scaled = [[v * occ[k] for v in value[k]] for k in range(2)]
        for p, (i, j) in enumerate(PAIRS):
            term = scaled[0][i] * value[0][j] + scaled[1][i] * value[1][j]
            word, at = divmod(STRIDE * t + p, 128)
            packed[word] = jnp.where(
                lane == at, jnp.sum(term, axis=1, keepdims=True), packed[word]
            )
    for k in range(out_ref.shape[0]):
        for word in range(3):
            out_ref[k, :, 128 * word:128 * (word + 1)] = packed[word]


def gram(occ, parts, peers):
    vmem = pl.BlockSpec(memory_space=pltpu.VMEM)
    return pl.pallas_call(
        gram_kernel,
        in_specs=[vmem] * 7,
        out_specs=vmem,
        out_shape=jax.ShapeDtypeStruct((peers, 8, 3 * 128), F32),
        compiler_params=pltpu.CompilerParams(vmem_limit_bytes=8 * 1024 * 1024),
        name="gram",
    )(occ, *parts)


def unfold_kernel(in_ref, out_ref):
    total = in_ref[0]
    for k in range(1, in_ref.shape[0]):
        total = total + in_ref[k]
    padded = jnp.concatenate([total, jnp.zeros((120, 3 * 128), F32)], axis=0)
    turned = jnp.transpose(padded)
    turned = jnp.concatenate(
        [turned[STRIDE * t:STRIDE * (t + 1), :8] for t in range(ATOMS_DEV // 8)], axis=1
    )
    place = {pair: p for p, pair in enumerate(PAIRS)}
    for i in range(NPROJ):
        first = place[(i, i)]
        out_ref[i, i:NPROJ, :] = turned[first:first + NPROJ - i]
        for j in range(i + 1, NPROJ):
            out_ref[j, i:i + 1, :] = turned[first + j - i:first + j - i + 1]


def unfold(everything):
    vmem = pl.BlockSpec(memory_space=pltpu.VMEM)
    return pl.pallas_call(
        unfold_kernel,
        in_specs=[vmem],
        out_specs=vmem,
        out_shape=jax.ShapeDtypeStruct((NPROJ, NPROJ, ATOMS_DEV), F32),
        compiler_params=pltpu.CompilerParams(vmem_limit_bytes=8 * 1024 * 1024),
        name="unfold",
    )(everything)


def body(wavefunctions, projectors, slot_atom, occupations):
    band_count = wavefunctions.shape[0]
    block_count, capacity, proj_count, block_len = projectors.shape
    domains = lax.axis_size("grid")
    peers = lax.axis_size("band")
    domain = lax.axis_index("grid").astype(jnp.int32).reshape(1)
    chips = domains // 2
    stored = jnp.transpose(projectors, (0, 2, 1, 3)).reshape(
        block_count, proj_count * capacity, block_len
    )
    slots = jnp.transpose(slot_atom)

    partner = [(i, i ^ 1) for i in range(domains)]
    along = [(2 * k + 1, (2 * k + 3) % domains) for k in range(chips)]
    along += [(2 * k, (2 * k - 2) % domains) for k in range(chips)]
    across = [(2 * k + 1, (2 * k + 2) % domains) for k in range(chips)]
    across += [(2 * k, (2 * k - 1) % domains) for k in range(chips)]

    def send(own, inner, outer, far):
        swapped = lax.ppermute(inner, "grid", partner)
        passed = lax.ppermute(far, "grid", along)
        near = own + swapped[0]
        first = outer[0] + swapped[1]
        second = outer[1] + swapped[2]
        near, first, second = lax.optimization_barrier((near, first, second))
        return near, lax.ppermute(second, "grid", along), first, passed, second

    def finish(first, passed):
        return lax.ppermute(first + passed, "grid", across)

    blocks = project(wavefunctions, stored, slots, domain, domains, 0)
    near, second, first, passed, sent = send(*blocks)
    blocks = project(
        wavefunctions, stored, slots, domain, domains, LANES, (sent,)
    )
    near1, second1, first1, passed1, _ = send(*blocks)
    last = finish(first, passed)
    last1 = finish(first1, passed1)
    parts = (near, second, last, near1, second1, last1)
    packed = gram(occupations.reshape(1, band_count), parts, peers)
    everything = lax.all_to_all(packed, "band", 0, 0, tiled=True)
    return jnp.transpose(unfold(everything), (2, 0, 1))


def solution(mesh):
    in_specs = (P("band", "grid"), P("grid", None, None, None), P("grid", None), P("band"))
    out_specs = P("grid", None, None)
    return jax.shard_map(body, mesh=mesh, in_specs=in_specs, out_specs=out_specs, check_vma=False)
```

```python
import functools

import jax
import jax.numpy as jnp
from jax import lax
from jax.experimental import pallas as pl
from jax.experimental.pallas import tpu as pltpu
from jax.sharding import PartitionSpec as P

REACH = 3
ATOMS_DEV = 32
NPROJ = 13
CAP = 8
BLK = 256
STRIDE = 96
PAIRS = [(i, j) for i in range(NPROJ) for j in range(i, NPROJ)]
F32 = jnp.float32
BF16 = jnp.bfloat16


def targets(slots, domain, domains):
    half = domains // 2
    owner = slots >> 5
    rel = ((owner - domain + half) & (domains - 1)) - half
    rel = jnp.where((domain & 1) == 1, rel, -rel)
    band = jnp.where(rel < 0, -rel, jnp.where(rel > 0, rel + REACH, 0))
    return jnp.where(slots >= 0, band * ATOMS_DEV + (slots & (ATOMS_DEV - 1)), 255)


def project_kernel(
    domain_ref, slot_hbm, proj_hbm, wave_hbm, own_ref, inner_ref, outer_ref, far_ref,
    slot_buf, wave_buf, proj_buf, turn_buf, term_buf, slot_sem, chunk_sem, *, domains,
):
    blocks = proj_hbm.shape[0]
    total = blocks * CAP
    sizes = chunk_sizes(blocks)
    starts = [sum(sizes[:c]) for c in range(len(sizes))]
    copies = [pltpu.make_async_copy(slot_hbm, slot_buf, slot_sem)]
    for c, (first, size) in enumerate(zip(starts, sizes)):
        rows = pl.ds(first, size)
        cols = pl.ds(first * BLK, size * BLK)
        copies.append(
            pltpu.make_async_copy(proj_hbm.at[rows], proj_buf.at[rows], chunk_sem.at[c])
        )
        copies.append(
            pltpu.make_async_copy(wave_hbm.at[:, cols], wave_buf.at[:, cols], chunk_sem.at[c])
        )
    copies[0].start()
    for copy in copies[1:]:
        copy.start(priority=1)

    def turn(c):
        rows = sizes[c] * (NPROJ * CAP + wave_hbm.shape[0]) // 3
        both = term_buf.at[:3, :rows, :]
        pltpu.make_async_copy(both, both, chunk_sem.at[c]).wait()
        for g in range(starts[c], starts[c] + sizes[c]):
            turn_buf[g] = wave_buf[:, g * BLK:(g + 1) * BLK].T

    parts = 4
    edges = [p * total // parts for p in range(parts + 1)]

    def multiply(c):
        for g in range(starts[c], starts[c] + sizes[c], 2):
            pair = [
                jnp.dot(proj_buf[k], turn_buf[k], preferred_element_type=F32) for k in (g, g + 1)
            ]
            part = max(p for p in range(parts) if edges[p] <= g * CAP)
            size = edges[part + 1] - edges[part]
            row = edges[part] + g * CAP
            for i in range(NPROJ):
                value = jnp.concatenate([p[i * CAP:(i + 1) * CAP] for p in pair], axis=0)
                high = value.astype(BF16)
                term_buf[i, row:row + 2 * CAP, :] = high
                term_buf[i, row + size:row + size + 2 * CAP, :] = (
                    value - high.astype(F32)
                ).astype(BF16)

    window = (2 * REACH + 1) * ATOMS_DEV

    def selectors():
        copies[0].wait()
        slot_rows = targets(slot_buf[...], domain_ref[0], domains).astype(F32).astype(BF16)
        spread = (
            lax.broadcasted_iota(jnp.int32, (blocks, total), 0)
            == lax.broadcasted_iota(jnp.int32, (blocks, total), 1) // CAP
        ).astype(F32).astype(BF16)
        wide = jnp.dot(slot_rows, spread, preferred_element_type=F32)
        keep = (
            lax.broadcasted_iota(jnp.int32, (CAP, total), 0)
            == lax.broadcasted_iota(jnp.int32, (CAP, total), 1) % CAP
        )
        row_of = jnp.sum(jnp.where(keep, wide, 0.0), axis=0, keepdims=True).astype(jnp.int32)
        return row_of

    def gather(row_of, part, kinds):
        size = edges[part + 1] - edges[part]
        one = (
            lax.broadcasted_iota(jnp.int32, (window, size), 0)
            == row_of[:, edges[part]:edges[part + 1]]
        ).astype(F32).astype(BF16)
        both = jnp.concatenate([one, one], axis=1)
        for i in kinds:
            result = jnp.dot(
                both, term_buf[i, 2 * edges[part]:2 * edges[part + 1], :],
                preferred_element_type=F32,
            )
            places = [(own_ref, (i,))]
            places += [(inner_ref, (k, i)) for k in range(REACH)]
            places += [(outer_ref, (k, i)) for k in range(REACH - 1)]
            places += [(far_ref, (i,))]
            for k, (ref, at) in enumerate(places):
                value = result[k * ATOMS_DEV:(k + 1) * ATOMS_DEV]
                ref[at] = value if part == 0 else ref[at] + value

    per_part = len(sizes) // parts
    row_of = None
    for step in range(len(sizes) + 1):
        if step < len(sizes):
            turn(step)
        if step > 0:
            multiply(step - 1)
        if step == 1:
            row_of = selectors()
        ready, turn_of = divmod(step - per_part, per_part)
        if 0 <= ready < parts - 1:
            gather(row_of, ready, range(NPROJ)[turn_of::per_part])
    gather(row_of, parts - 1, range(NPROJ))


def chunk_sizes(blocks):
    return [blocks // 8] * 8


def project(wave, proj, slots, domain, domains):
    bands, points = wave.shape
    blocks = proj.shape[0]
    chunks = len(chunk_sizes(blocks))
    block = (NPROJ, ATOMS_DEV, bands)
    vmem = pl.BlockSpec(memory_space=pltpu.VMEM)
    hbm = pl.BlockSpec(memory_space=pltpu.HBM)
    slots = pltpu.with_memory_space_constraint(slots, pltpu.HBM)
    return pl.pallas_call(
        functools.partial(project_kernel, domains=domains),
        in_specs=[pl.BlockSpec(memory_space=pltpu.SMEM), hbm, hbm, hbm],
        out_specs=[vmem] * 4,
        out_shape=[
            jax.ShapeDtypeStruct(block, F32),
            jax.ShapeDtypeStruct((REACH,) + block, F32),
            jax.ShapeDtypeStruct((REACH - 1,) + block, F32),
            jax.ShapeDtypeStruct(block, F32),
        ],
        scratch_shapes=[
            pltpu.VMEM(slots.shape, jnp.int32),
            pltpu.VMEM((bands, points), BF16),
            pltpu.VMEM((blocks, NPROJ * CAP, BLK), BF16),
            pltpu.VMEM((blocks, BLK, bands), BF16),
            pltpu.VMEM((NPROJ, 2 * blocks * CAP, bands), BF16),
            pltpu.SemaphoreType.DMA,
            pltpu.SemaphoreType.DMA((chunks,)),
        ],
        compiler_params=pltpu.CompilerParams(vmem_limit_bytes=48 * 1024 * 1024),
        name="project",
    )(domain, slots, proj, wave)


def gram_kernel(occ_ref, a_ref, b_ref, c_ref, out_ref):
    peers = out_ref.shape[0]
    occ = occ_ref[...]
    lane = lax.broadcasted_iota(jnp.int32, (8, 128), 1)
    packed = [jnp.zeros((8, 128), F32) for _ in range(3)]
    for t in range(ATOMS_DEV // 8):
        rows = slice(8 * t, 8 * t + 8)
        value = [a_ref[i, rows, :] + b_ref[i, rows, :] + c_ref[i, rows, :] for i in range(NPROJ)]
        scaled = [v * occ for v in value]
        for p, (i, j) in enumerate(PAIRS):
            term = jnp.sum(scaled[i] * value[j], axis=1, keepdims=True)
            word, at = divmod(STRIDE * t + p, 128)
            packed[word] = jnp.where(lane == at, term, packed[word])
    for k in range(peers):
        for word in range(3):
            out_ref[k, :, 128 * word:128 * (word + 1)] = packed[word]


def gram(occ, a, b, c, peers):
    vmem = pl.BlockSpec(memory_space=pltpu.VMEM)
    return pl.pallas_call(
        gram_kernel,
        in_specs=[vmem] * 4,
        out_specs=vmem,
        out_shape=jax.ShapeDtypeStruct((peers, 8, 3 * 128), F32),
        compiler_params=pltpu.CompilerParams(vmem_limit_bytes=8 * 1024 * 1024),
        name="gram",
    )(occ, a, b, c)


def unfold_kernel(in_ref, out_ref):
    total = in_ref[0]
    for k in range(1, in_ref.shape[0]):
        total = total + in_ref[k]
    padded = jnp.concatenate([total, jnp.zeros((120, 3 * 128), F32)], axis=0)
    turned = jnp.transpose(padded)
    turned = jnp.concatenate(
        [turned[STRIDE * t:STRIDE * (t + 1), :8] for t in range(ATOMS_DEV // 8)], axis=1
    )
    place = {pair: p for p, pair in enumerate(PAIRS)}
    for i in range(NPROJ):
        first = place[(i, i)]
        out_ref[i, i:NPROJ, :] = turned[first:first + NPROJ - i]
        for j in range(i + 1, NPROJ):
            out_ref[j, i:i + 1, :] = turned[first + j - i:first + j - i + 1]


def unfold(everything):
    vmem = pl.BlockSpec(memory_space=pltpu.VMEM)
    return pl.pallas_call(
        unfold_kernel,
        in_specs=[vmem],
        out_specs=vmem,
        out_shape=jax.ShapeDtypeStruct((NPROJ, NPROJ, ATOMS_DEV), F32),
        compiler_params=pltpu.CompilerParams(vmem_limit_bytes=8 * 1024 * 1024),
        name="unfold",
    )(everything)


def body(wavefunctions, projectors, slot_atom, occupations):
    band_count = wavefunctions.shape[0]
    block_count, capacity, proj_count, block_len = projectors.shape
    domains = lax.axis_size("grid")
    peers = lax.axis_size("band")
    domain = lax.axis_index("grid").astype(jnp.int32).reshape(1)
    chips = domains // 2
    stored = jnp.transpose(projectors, (0, 2, 1, 3)).reshape(
        block_count, proj_count * capacity, block_len
    )
    own, inner, outer, far = project(
        wavefunctions, stored, jnp.transpose(slot_atom), domain, domains
    )

    partner = [(i, i ^ 1) for i in range(domains)]
    along = [(2 * k + 1, (2 * k + 3) % domains) for k in range(chips)]
    along += [(2 * k, (2 * k - 2) % domains) for k in range(chips)]
    across = [(2 * k + 1, (2 * k + 2) % domains) for k in range(chips)]
    across += [(2 * k, (2 * k - 1) % domains) for k in range(chips)]

    swapped = lax.ppermute(inner, "grid", partner)
    passed = lax.ppermute(far, "grid", along)
    near = own + swapped[0]
    first = outer[0] + swapped[1]
    second = outer[1] + swapped[2]
    near, first, second = lax.optimization_barrier((near, first, second))
    final_second = lax.ppermute(second, "grid", along)
    first = first + passed
    final_first = lax.ppermute(first, "grid", across)

    occ = occupations.reshape(1, band_count)
    packed = gram(occ, near, final_second, final_first, peers)
    everything = lax.all_to_all(packed, "band", 0, 0, tiled=True)
    return jnp.transpose(unfold(everything), (2, 0, 1))


def solution(mesh):
    in_specs = (P("band", "grid"), P("grid", None, None, None), P("grid", None), P("band"))
    out_specs = P("grid", None, None)
    return jax.shard_map(body, mesh=mesh, in_specs=in_specs, out_specs=out_specs, check_vma=False)
```

```python
import functools

import jax
import jax.numpy as jnp
from jax import lax
from jax.experimental import pallas as pl
from jax.experimental.pallas import tpu as pltpu
from jax.sharding import PartitionSpec as P

REACH = 3
ATOMS_DEV = 32
NPROJ = 13
CAP = 8
BLK = 256
STRIDE = 96
PAIRS = [(i, j) for i in range(NPROJ) for j in range(i, NPROJ)]
F32 = jnp.float32
BF16 = jnp.bfloat16


def targets(slots, domain, domains):
    half = domains // 2
    owner = slots >> 5
    rel = ((owner - domain + half) & (domains - 1)) - half
    rel = jnp.where((domain & 1) == 1, rel, -rel)
    band = jnp.where(rel < 0, -rel, jnp.where(rel > 0, rel + REACH, 0))
    return jnp.where(slots >= 0, band * ATOMS_DEV + (slots & (ATOMS_DEV - 1)), 255)


def project_kernel(
    domain_ref, slot_hbm, proj_hbm, wave_hbm, own_ref, inner_ref, outer_ref, far_ref,
    slot_buf, wave_buf, proj_buf, turn_buf, term_buf, slot_sem, chunk_sem, *, domains,
):
    blocks = proj_hbm.shape[0]
    total = blocks * CAP
    sizes = chunk_sizes(blocks)
    starts = [sum(sizes[:c]) for c in range(len(sizes))]
    copies = [pltpu.make_async_copy(slot_hbm, slot_buf, slot_sem)]
    for c, (first, size) in enumerate(zip(starts, sizes)):
        rows = pl.ds(first, size)
        cols = pl.ds(first * BLK, size * BLK)
        copies.append(
            pltpu.make_async_copy(proj_hbm.at[rows], proj_buf.at[rows], chunk_sem.at[c])
        )
        copies.append(
            pltpu.make_async_copy(wave_hbm.at[:, cols], wave_buf.at[:, cols], chunk_sem.at[c])
        )
    copies[0].start()
    for copy in copies[1:]:
        copy.start(priority=1)

    def arrive(c):
        rows = sizes[c] * (NPROJ * CAP + wave_hbm.shape[0]) // 3
        both = term_buf.at[:3, :rows, :]
        pltpu.make_async_copy(both, both, chunk_sem.at[c]).wait()

    def turn(c, q):
        for g in range(starts[c] + 2 * q, starts[c] + 2 * q + 2):
            turn_buf[g] = wave_buf[:, g * BLK:(g + 1) * BLK].T

    parts = 4
    edges = [p * total // parts for p in range(parts + 1)]

    def multiply(c, q):
        for g in range(starts[c] + 2 * q, starts[c] + 2 * q + 2, 2):
            pair = [
                jnp.dot(proj_buf[k], turn_buf[k], preferred_element_type=F32) for k in (g, g + 1)
            ]
            part = max(p for p in range(parts) if edges[p] <= g * CAP)
            size = edges[part + 1] - edges[part]
            row = edges[part] + g * CAP
            for i in range(NPROJ):
                value = jnp.concatenate([p[i * CAP:(i + 1) * CAP] for p in pair], axis=0)
                high = value.astype(BF16)
                term_buf[i, row:row + 2 * CAP, :] = high
                term_buf[i, row + size:row + size + 2 * CAP, :] = (
                    value - high.astype(F32)
                ).astype(BF16)

    window = (2 * REACH + 1) * ATOMS_DEV

    def selectors():
        copies[0].wait()
        slot_rows = targets(slot_buf[...], domain_ref[0], domains).astype(F32).astype(BF16)
        spread = (
            lax.broadcasted_iota(jnp.int32, (blocks, total), 0)
            == lax.broadcasted_iota(jnp.int32, (blocks, total), 1) // CAP
        ).astype(F32).astype(BF16)
        wide = jnp.dot(slot_rows, spread, preferred_element_type=F32)
        keep = (
            lax.broadcasted_iota(jnp.int32, (CAP, total), 0)
            == lax.broadcasted_iota(jnp.int32, (CAP, total), 1) % CAP
        )
        row_of = jnp.sum(jnp.where(keep, wide, 0.0), axis=0, keepdims=True).astype(jnp.int32)
        return row_of

    def gather(row_of, part, kinds):
        size = edges[part + 1] - edges[part]
        one = (
            lax.broadcasted_iota(jnp.int32, (window, size), 0)
            == row_of[:, edges[part]:edges[part + 1]]
        ).astype(F32).astype(BF16)
        both = jnp.concatenate([one, one], axis=1)
        for i in kinds:
            result = jnp.dot(
                both, term_buf[i, 2 * edges[part]:2 * edges[part + 1], :],
                preferred_element_type=F32,
            )
            places = [(own_ref, (i,))]
            places += [(inner_ref, (k, i)) for k in range(REACH)]
            places += [(outer_ref, (k, i)) for k in range(REACH - 1)]
            places += [(far_ref, (i,))]
            for k, (ref, at) in enumerate(places):
                value = result[k * ATOMS_DEV:(k + 1) * ATOMS_DEV]
                ref[at] = value if part == 0 else ref[at] + value

    per_part = len(sizes) // parts
    row_of = None
    for step in range(len(sizes) + 1):
        if step < len(sizes):
            arrive(step)
        if step == 1:
            row_of = selectors()
        ready, turn_of = divmod(step - per_part - 1, per_part)
        kinds = list(range(NPROJ))[turn_of::per_part] if 0 <= ready < parts - 1 else []
        count = sizes[0] // 2
        for q in range(count):
            if step > 0:
                multiply(step - 1, q)
            if kinds[q::count]:
                gather(row_of, ready, kinds[q::count])
            if step < len(sizes):
                turn(step, q)
    gather(row_of, parts - 1, range(NPROJ))


def chunk_sizes(blocks):
    return [blocks // 8] * 8


def project(wave, proj, slots, domain, domains):
    bands, points = wave.shape
    blocks = proj.shape[0]
    chunks = len(chunk_sizes(blocks))
    block = (NPROJ, ATOMS_DEV, bands)
    vmem = pl.BlockSpec(memory_space=pltpu.VMEM)
    hbm = pl.BlockSpec(memory_space=pltpu.HBM)
    slots = pltpu.with_memory_space_constraint(slots, pltpu.HBM)
    return pl.pallas_call(
        functools.partial(project_kernel, domains=domains),
        in_specs=[pl.BlockSpec(memory_space=pltpu.SMEM), hbm, hbm, hbm],
        out_specs=[vmem] * 4,
        out_shape=[
            jax.ShapeDtypeStruct(block, F32),
            jax.ShapeDtypeStruct((REACH,) + block, F32),
            jax.ShapeDtypeStruct((REACH - 1,) + block, F32),
            jax.ShapeDtypeStruct(block, F32),
        ],
        scratch_shapes=[
            pltpu.VMEM(slots.shape, jnp.int32),
            pltpu.VMEM((bands, points), BF16),
            pltpu.VMEM((blocks, NPROJ * CAP, BLK), BF16),
            pltpu.VMEM((blocks, BLK, bands), BF16),
            pltpu.VMEM((NPROJ, 2 * blocks * CAP, bands), BF16),
            pltpu.SemaphoreType.DMA,
            pltpu.SemaphoreType.DMA((chunks,)),
        ],
        compiler_params=pltpu.CompilerParams(vmem_limit_bytes=48 * 1024 * 1024),
        name="project",
    )(domain, slots, proj, wave)


def gram_kernel(occ_ref, a_ref, b_ref, c_ref, out_ref):
    peers = out_ref.shape[0]
    occ = occ_ref[...]
    lane = lax.broadcasted_iota(jnp.int32, (8, 128), 1)
    packed = [jnp.zeros((8, 128), F32) for _ in range(3)]
    for t in range(ATOMS_DEV // 8):
        rows = slice(8 * t, 8 * t + 8)
        value = [a_ref[i, rows, :] + b_ref[i, rows, :] + c_ref[i, rows, :] for i in range(NPROJ)]
        scaled = [v * occ for v in value]
        for p, (i, j) in enumerate(PAIRS):
            term = jnp.sum(scaled[i] * value[j], axis=1, keepdims=True)
            word, at = divmod(STRIDE * t + p, 128)
            packed[word] = jnp.where(lane == at, term, packed[word])
    for k in range(peers):
        for word in range(3):
            out_ref[k, :, 128 * word:128 * (word + 1)] = packed[word]


def gram(occ, a, b, c, peers):
    vmem = pl.BlockSpec(memory_space=pltpu.VMEM)
    return pl.pallas_call(
        gram_kernel,
        in_specs=[vmem] * 4,
        out_specs=vmem,
        out_shape=jax.ShapeDtypeStruct((peers, 8, 3 * 128), F32),
        compiler_params=pltpu.CompilerParams(vmem_limit_bytes=8 * 1024 * 1024),
        name="gram",
    )(occ, a, b, c)


def unfold_kernel(in_ref, out_ref):
    total = in_ref[0]
    for k in range(1, in_ref.shape[0]):
        total = total + in_ref[k]
    padded = jnp.concatenate([total, jnp.zeros((120, 3 * 128), F32)], axis=0)
    turned = jnp.transpose(padded)
    turned = jnp.concatenate(
        [turned[STRIDE * t:STRIDE * (t + 1), :8] for t in range(ATOMS_DEV // 8)], axis=1
    )
    place = {pair: p for p, pair in enumerate(PAIRS)}
    for i in range(NPROJ):
        first = place[(i, i)]
        out_ref[i, i:NPROJ, :] = turned[first:first + NPROJ - i]
        for j in range(i + 1, NPROJ):
            out_ref[j, i:i + 1, :] = turned[first + j - i:first + j - i + 1]


def unfold(everything):
    vmem = pl.BlockSpec(memory_space=pltpu.VMEM)
    return pl.pallas_call(
        unfold_kernel,
        in_specs=[vmem],
        out_specs=vmem,
        out_shape=jax.ShapeDtypeStruct((NPROJ, NPROJ, ATOMS_DEV), F32),
        compiler_params=pltpu.CompilerParams(vmem_limit_bytes=8 * 1024 * 1024),
        name="unfold",
    )(everything)


def body(wavefunctions, projectors, slot_atom, occupations):
    band_count = wavefunctions.shape[0]
    block_count, capacity, proj_count, block_len = projectors.shape
    domains = lax.axis_size("grid")
    peers = lax.axis_size("band")
    domain = lax.axis_index("grid").astype(jnp.int32).reshape(1)
    chips = domains // 2
    stored = jnp.transpose(projectors, (0, 2, 1, 3)).reshape(
        block_count, proj_count * capacity, block_len
    )
    own, inner, outer, far = project(
        wavefunctions, stored, jnp.transpose(slot_atom), domain, domains
    )

    partner = [(i, i ^ 1) for i in range(domains)]
    along = [(2 * k + 1, (2 * k + 3) % domains) for k in range(chips)]
    along += [(2 * k, (2 * k - 2) % domains) for k in range(chips)]
    across = [(2 * k + 1, (2 * k + 2) % domains) for k in range(chips)]
    across += [(2 * k, (2 * k - 1) % domains) for k in range(chips)]

    swapped = lax.ppermute(inner, "grid", partner)
    passed = lax.ppermute(far, "grid", along)
    near = own + swapped[0]
    first = outer[0] + swapped[1]
    second = outer[1] + swapped[2]
    near, first, second = lax.optimization_barrier((near, first, second))
    final_second = lax.ppermute(second, "grid", along)
    first = first + passed
    final_first = lax.ppermute(first, "grid", across)

    occ = occupations.reshape(1, band_count)
    packed = gram(occ, near, final_second, final_first, peers)
    everything = lax.all_to_all(packed, "band", 0, 0, tiled=True)
    return jnp.transpose(unfold(everything), (2, 0, 1))


def solution(mesh):
    in_specs = (P("band", "grid"), P("grid", None, None, None), P("grid", None), P("band"))
    out_specs = P("grid", None, None)
    return jax.shard_map(body, mesh=mesh, in_specs=in_specs, out_specs=out_specs, check_vma=False)
```

```python
import functools

import jax
import jax.numpy as jnp
from jax import lax
from jax.experimental import pallas as pl
from jax.experimental.pallas import tpu as pltpu
from jax.sharding import PartitionSpec as P

REACH = 3
ATOMS_DEV = 32
NPROJ = 13
CAP = 8
BLK = 256
STRIDE = 96
PAIRS = [(i, j) for i in range(NPROJ) for j in range(i, NPROJ)]
F32 = jnp.float32
BF16 = jnp.bfloat16


def targets(slots, domain, domains):
    half = domains // 2
    owner = slots >> 5
    rel = ((owner - domain + half) & (domains - 1)) - half
    rel = jnp.where((domain & 1) == 1, rel, -rel)
    band = jnp.where(rel < 0, -rel, jnp.where(rel > 0, rel + REACH, 0))
    return jnp.where(slots >= 0, band * ATOMS_DEV + (slots & (ATOMS_DEV - 1)), 255)


def project_kernel(
    domain_ref, slot_hbm, proj_hbm, wave_hbm, own_ref, inner_ref, outer_ref, far_ref,
    slot_buf, wave_buf, proj_buf, turn_buf, term_buf, slot_sem, chunk_sem, *, domains,
):
    blocks = proj_hbm.shape[0]
    total = blocks * CAP
    sizes = chunk_sizes(blocks)
    starts = [sum(sizes[:c]) for c in range(len(sizes))]
    copies = [pltpu.make_async_copy(slot_hbm, slot_buf, slot_sem)]
    arriving = []
    for c in range(len(sizes)):
        cols = pl.ds(starts[c] * BLK, sizes[c] * BLK)
        kept = [c - 1] if c else []
        kept += [c] if c == len(sizes) - 1 else []
        for k in kept:
            rows = pl.ds(starts[k], sizes[k])
            copies.append(
                pltpu.make_async_copy(proj_hbm.at[rows], proj_buf.at[rows], chunk_sem.at[c])
            )
        copies.append(
            pltpu.make_async_copy(wave_hbm.at[:, cols], wave_buf.at[:, cols], chunk_sem.at[c])
        )
        arriving.append(
            sizes[c] * wave_hbm.shape[0] + sum(sizes[k] for k in kept) * NPROJ * CAP
        )
    copies[0].start()
    for copy in copies[1:]:
        copy.start(priority=1)

    def arrive(c):
        deep = 4 if arriving[c] % 64 == 0 else 3
        both = term_buf.at[:deep, :arriving[c] // deep, :]
        pltpu.make_async_copy(both, both, chunk_sem.at[c]).wait()

    def turn(c, q):
        for g in range(starts[c] + 2 * q, starts[c] + 2 * q + 2):
            turn_buf[g] = wave_buf[:, g * BLK:(g + 1) * BLK].T

    parts = 4
    edges = [p * total // parts for p in range(parts + 1)]

    def multiply(c, q):
        for g in range(starts[c] + 2 * q, starts[c] + 2 * q + 2, 2):
            pair = [
                jnp.dot(proj_buf[k], turn_buf[k], preferred_element_type=F32) for k in (g, g + 1)
            ]
            part = max(p for p in range(parts) if edges[p] <= g * CAP)
            size = edges[part + 1] - edges[part]
            row = edges[part] + g * CAP
            for i in range(NPROJ):
                value = jnp.concatenate([p[i * CAP:(i + 1) * CAP] for p in pair], axis=0)
                high = value.astype(BF16)
                term_buf[i, row:row + 2 * CAP, :] = high
                term_buf[i, row + size:row + size + 2 * CAP, :] = (
                    value - high.astype(F32)
                ).astype(BF16)

    window = (2 * REACH + 1) * ATOMS_DEV

    def selectors():
        copies[0].wait()
        slot_rows = targets(slot_buf[...], domain_ref[0], domains).astype(F32).astype(BF16)
        spread = (
            lax.broadcasted_iota(jnp.int32, (blocks, total), 0)
            == lax.broadcasted_iota(jnp.int32, (blocks, total), 1) // CAP
        ).astype(F32).astype(BF16)
        wide = jnp.dot(slot_rows, spread, preferred_element_type=F32)
        keep = (
            lax.broadcasted_iota(jnp.int32, (CAP, total), 0)
            == lax.broadcasted_iota(jnp.int32, (CAP, total), 1) % CAP
        )
        row_of = jnp.sum(jnp.where(keep, wide, 0.0), axis=0, keepdims=True).astype(jnp.int32)
        return row_of

    def gather(row_of, part, kinds):
        size = edges[part + 1] - edges[part]
        one = (
            lax.broadcasted_iota(jnp.int32, (window, size), 0)
            == row_of[:, edges[part]:edges[part + 1]]
        ).astype(F32).astype(BF16)
        both = jnp.concatenate([one, one], axis=1)
        for i in kinds:
            result = jnp.dot(
                both, term_buf[i, 2 * edges[part]:2 * edges[part + 1], :],
                preferred_element_type=F32,
            )
            places = [(own_ref, (i,))]
            places += [(inner_ref, (k, i)) for k in range(REACH)]
            places += [(outer_ref, (k, i)) for k in range(REACH - 1)]
            places += [(far_ref, (i,))]
            for k, (ref, at) in enumerate(places):
                value = result[k * ATOMS_DEV:(k + 1) * ATOMS_DEV]
                ref[at] = value if part == 0 else ref[at] + value

    per_part = len(sizes) // parts
    row_of = None
    for step in range(len(sizes) + 1):
        if step < len(sizes):
            arrive(step)
        if step == 1:
            row_of = selectors()
        ready, turn_of = divmod(step - per_part - 1, per_part)
        kinds = list(range(NPROJ))[turn_of::per_part] if 0 <= ready < parts - 1 else []
        count = sizes[0] // 2
        for q in range(count):
            if step > 0:
                multiply(step - 1, q)
            if kinds[q::count]:
                gather(row_of, ready, kinds[q::count])
            if step < len(sizes):
                turn(step, q)
    gather(row_of, parts - 1, range(NPROJ))


def chunk_sizes(blocks):
    return [blocks // 8] * 8


def project(wave, proj, slots, domain, domains):
    bands, points = wave.shape
    blocks = proj.shape[0]
    chunks = len(chunk_sizes(blocks))
    block = (NPROJ, ATOMS_DEV, bands)
    vmem = pl.BlockSpec(memory_space=pltpu.VMEM)
    hbm = pl.BlockSpec(memory_space=pltpu.HBM)
    slots = pltpu.with_memory_space_constraint(slots, pltpu.HBM)
    return pl.pallas_call(
        functools.partial(project_kernel, domains=domains),
        in_specs=[pl.BlockSpec(memory_space=pltpu.SMEM), hbm, hbm, hbm],
        out_specs=[vmem] * 4,
        out_shape=[
            jax.ShapeDtypeStruct(block, F32),
            jax.ShapeDtypeStruct((REACH,) + block, F32),
            jax.ShapeDtypeStruct((REACH - 1,) + block, F32),
            jax.ShapeDtypeStruct(block, F32),
        ],
        scratch_shapes=[
            pltpu.VMEM(slots.shape, jnp.int32),
            pltpu.VMEM((bands, points), BF16),
            pltpu.VMEM((blocks, NPROJ * CAP, BLK), BF16),
            pltpu.VMEM((blocks, BLK, bands), BF16),
            pltpu.VMEM((NPROJ, 2 * blocks * CAP, bands), BF16),
            pltpu.SemaphoreType.DMA,
            pltpu.SemaphoreType.DMA((chunks,)),
        ],
        compiler_params=pltpu.CompilerParams(vmem_limit_bytes=48 * 1024 * 1024),
        name="project",
    )(domain, slots, proj, wave)


def gram_kernel(occ_ref, a_ref, b_ref, c_ref, out_ref):
    peers = out_ref.shape[0]
    occ = occ_ref[...]
    lane = lax.broadcasted_iota(jnp.int32, (8, 128), 1)
    packed = [jnp.zeros((8, 128), F32) for _ in range(3)]
    for t in range(ATOMS_DEV // 8):
        rows = slice(8 * t, 8 * t + 8)
        value = [a_ref[i, rows, :] + b_ref[i, rows, :] + c_ref[i, rows, :] for i in range(NPROJ)]
        scaled = [v * occ for v in value]
        for p, (i, j) in enumerate(PAIRS):
            term = jnp.sum(scaled[i] * value[j], axis=1, keepdims=True)
            word, at = divmod(STRIDE * t + p, 128)
            packed[word] = jnp.where(lane == at, term, packed[word])
    for k in range(peers):
        for word in range(3):
            out_ref[k, :, 128 * word:128 * (word + 1)] = packed[word]


def gram(occ, a, b, c, peers):
    vmem = pl.BlockSpec(memory_space=pltpu.VMEM)
    return pl.pallas_call(
        gram_kernel,
        in_specs=[vmem] * 4,
        out_specs=vmem,
        out_shape=jax.ShapeDtypeStruct((peers, 8, 3 * 128), F32),
        compiler_params=pltpu.CompilerParams(vmem_limit_bytes=8 * 1024 * 1024),
        name="gram",
    )(occ, a, b, c)


def unfold_kernel(in_ref, out_ref):
    total = in_ref[0]
    for k in range(1, in_ref.shape[0]):
        total = total + in_ref[k]
    padded = jnp.concatenate([total, jnp.zeros((120, 3 * 128), F32)], axis=0)
    turned = jnp.transpose(padded)
    turned = jnp.concatenate(
        [turned[STRIDE * t:STRIDE * (t + 1), :8] for t in range(ATOMS_DEV // 8)], axis=1
    )
    place = {pair: p for p, pair in enumerate(PAIRS)}
    for i in range(NPROJ):
        first = place[(i, i)]
        out_ref[i, i:NPROJ, :] = turned[first:first + NPROJ - i]
        for j in range(i + 1, NPROJ):
            out_ref[j, i:i + 1, :] = turned[first + j - i:first + j - i + 1]


def unfold(everything):
    vmem = pl.BlockSpec(memory_space=pltpu.VMEM)
    return pl.pallas_call(
        unfold_kernel,
        in_specs=[vmem],
        out_specs=vmem,
        out_shape=jax.ShapeDtypeStruct((NPROJ, NPROJ, ATOMS_DEV), F32),
        compiler_params=pltpu.CompilerParams(vmem_limit_bytes=8 * 1024 * 1024),
        name="unfold",
    )(everything)


def body(wavefunctions, projectors, slot_atom, occupations):
    band_count = wavefunctions.shape[0]
    block_count, capacity, proj_count, block_len = projectors.shape
    domains = lax.axis_size("grid")
    peers = lax.axis_size("band")
    domain = lax.axis_index("grid").astype(jnp.int32).reshape(1)
    chips = domains // 2
    stored = jnp.transpose(projectors, (0, 2, 1, 3)).reshape(
        block_count, proj_count * capacity, block_len
    )
    own, inner, outer, far = project(
        wavefunctions, stored, jnp.transpose(slot_atom), domain, domains
    )

    partner = [(i, i ^ 1) for i in range(domains)]
    along = [(2 * k + 1, (2 * k + 3) % domains) for k in range(chips)]
    along += [(2 * k, (2 * k - 2) % domains) for k in range(chips)]
    across = [(2 * k + 1, (2 * k + 2) % domains) for k in range(chips)]
    across += [(2 * k, (2 * k - 1) % domains) for k in range(chips)]

    swapped = lax.ppermute(inner, "grid", partner)
    passed = lax.ppermute(far, "grid", along)
    near = own + swapped[0]
    first = outer[0] + swapped[1]
    second = outer[1] + swapped[2]
    near, first, second = lax.optimization_barrier((near, first, second))
    final_second = lax.ppermute(second, "grid", along)
    first = first + passed
    final_first = lax.ppermute(first, "grid", across)

    occ = occupations.reshape(1, band_count)
    packed = gram(occ, near, final_second, final_first, peers)
    everything = lax.all_to_all(packed, "band", 0, 0, tiled=True)
    return jnp.transpose(unfold(everything), (2, 0, 1))


def solution(mesh):
    in_specs = (P("band", "grid"), P("grid", None, None, None), P("grid", None), P("band"))
    out_specs = P("grid", None, None)
    return jax.shard_map(body, mesh=mesh, in_specs=in_specs, out_specs=out_specs, check_vma=False)
```
